256 devices in a mesh: band: 32 (over z, x_hi, core), lane: 8 (over y, x_lo).
Axes of the slice: x: 4 (x_hi: 2, x_lo: 2; x = x_hi * 2 + x_lo), y: 4, z: 8, core: 2. Of those that a mesh axis runs over, the one named last changes fastest.
Arguments:
- load_terms: float32 [2048, 512, 256], P('band', 'lane'), may hold values from -6 to 6
- start_values: float32 [2048, 512, 256], P('band', 'lane'), may hold values from -6 to 6
- reaction_rate: float32 [2048, 512, 256], P('band', 'lane'), may hold values from 0.1 to 0.9
Outputs:
- solution: float32 [2048, 512, 256], P('band', 'lane')
- remaining: float32 [2048, 512, 256], P('band', 'lane')
The draws below stay inside these ranges and needn't reach their ends.
All inputs are finite; a program needn't handle non-finite values.
Results may differ from the reference program's by a relative error of at most 0.0003.
Values sent between devices are 32-bit elements.
A program may use at most 128 MiB of HBM per device.

```python
import jax
import jax.numpy as jnp
from jax import lax

LAYERS = 256
RATIO = 2
BEFORE = 3
AFTER = 2
INNER = 13
GRID_Y = 2048
GRID_X = 512


def levels(key, dims, shards, smallest, high):
    factor_of, own = 1.0, jax.random.fold_in(key, 6)
    for axis_at, shards_of in shards:
        steps = jnp.exp(jax.random.uniform(jax.random.fold_in(own, axis_at), (shards_of,), jnp.float32, smallest / len(shards), high / len(shards)))
        factor_of = factor_of * jnp.repeat(steps, dims[axis_at] // shards_of).reshape([-1 if axis == axis_at else 1 for axis in range(len(dims))])
    return factor_of


def gaussian(own_key, shape, width, bound, cuts=(), kind=jnp.bfloat16):
    level = levels(own_key, shape, cuts, -0.22, 0.18) if cuts else 1.0
    entries = jax.random.normal(own_key, shape, jnp.float32) * width * level
    return jnp.minimum(jnp.maximum(entries, -bound), bound).astype(kind)


def setup_inputs(seed: int = 0) -> dict:
    seeds = jax.random.split(jax.random.key(seed), 4)
    load_terms = gaussian(seeds[0], (GRID_Y, GRID_X, LAYERS), 1.0, 6.0, ((0, 32), (1, 8)), jnp.float32)
    start_values = gaussian(seeds[1], (GRID_Y, GRID_X, LAYERS), 1.0, 6.0, ((0, 32), (1, 8)), jnp.float32)
    reaction_rate = jnp.clip(0.1 + 0.79999997 * jax.random.uniform(seeds[2], (GRID_Y, GRID_X, LAYERS), jnp.float32) ** levels(seeds[2], (GRID_Y, GRID_X, LAYERS), ((0, 32), (1, 8)), -0.2, 0.2), 0.1, 0.9)
    return dict(load_terms=load_terms, start_values=start_values, reaction_rate=reaction_rate)


def cross_sum(padded):
    inner_y, inner_x = padded.shape[0] - 2, padded.shape[1] - 2
    middle_rows = lax.slice_in_dim(padded, 1, 1 + inner_y, axis=0)
    middle_columns = lax.slice_in_dim(padded, 1, 1 + inner_x, axis=1)
    return (lax.slice_in_dim(middle_columns, 0, inner_y, axis=0) + lax.slice_in_dim(middle_columns, 2, 2 + inner_y, axis=0)
            + lax.slice_in_dim(middle_rows, 0, inner_x, axis=1) + lax.slice_in_dim(middle_rows, 2, 2 + inner_x, axis=1))


def smooth_step(padded, values, load, mass_here):
    return values + 0.8 * (load + cross_sum(padded) - (4.0 + mass_here) * values) / (4.0 + mass_here)


def block_means(values):
    cut = values.reshape(values.shape[0] // RATIO, RATIO, values.shape[1] // RATIO, RATIO, values.shape[2])
    return jnp.mean(cut, axis=(1, 3))


def spread_blocks(values):
    return jnp.repeat(jnp.repeat(values, RATIO, axis=0), RATIO, axis=1)


def reference(load_terms, start_values, reaction_rate):
    values = start_values
    for sweep in range(BEFORE):
        values = smooth_step(jnp.pad(values, ((1, 1), (1, 1), (0, 0)), mode="constant"), values, load_terms, reaction_rate)
    defect = load_terms + cross_sum(jnp.pad(values, ((1, 1), (1, 1), (0, 0)), mode="constant")) - (4.0 + reaction_rate) * values
    coarse_load, coarse_mass = block_means(defect) * RATIO, block_means(reaction_rate) * RATIO
    coarse_values = jnp.zeros_like(coarse_load)
    for sweep in range(INNER):
        coarse_values = smooth_step(jnp.pad(coarse_values, ((1, 1), (1, 1), (0, 0)), mode="constant"), coarse_values, coarse_load, coarse_mass)
    values = values + spread_blocks(coarse_values)
    for sweep in range(AFTER):
        values = smooth_step(jnp.pad(values, ((1, 1), (1, 1), (0, 0)), mode="constant"), values, load_terms, reaction_rate)
    solution = values
    remaining = load_terms + cross_sum(jnp.pad(solution, ((1, 1), (1, 1), (0, 0)), mode="constant")) - (4.0 + reaction_rate) * solution
    return solution, remaining
```

```python
import functools

import jax
import jax.numpy as jnp
from jax import lax
from jax.experimental import pallas as pl
from jax.experimental.pallas import tpu as pltpu
from jax.sharding import PartitionSpec as P

BEFORE = 3
AFTER = 2
INNER = 13
OMEGA = 0.8
LANES = 128
DEPTH = 4
PAD = 8
CX = 16
MESH = pl.DeviceIdType.MESH


def kernel(
    bands, lanes, load_hbm, start_hbm, rate_hbm, u, w,
    f, diag, pair, cu, cl, cw, col_out, col_in, ccol_out, ccol_in, crow_in,
    in_sem, send_sem, recv_sem, csend_sem, crecv_sem,
):
    ny, nx = f.shape[1], f.shape[2]
    my, mx = ny // 2, nx // 2
    chunks = f.shape[0]
    wide = mx + 2 * PAD
    band, lane = lax.axis_index("band"), lax.axis_index("lane")
    near = (
        (band > 0, {"band": band - 1}),
        (band < bands - 1, {"band": band + 1}),
        (lane > 0, {"lane": lane - 1}),
        (lane < lanes - 1, {"lane": lane + 1}),
    )
    fine_x = pl.ds(PAD, nx)

    def loads(c):
        part = pl.ds(c * LANES, LANES)
        return (
            pltpu.make_async_copy(start_hbm.at[:, :, part], u.at[0, c, pl.ds(1, ny), fine_x], in_sem.at[c, 0]),
            pltpu.make_async_copy(rate_hbm.at[:, :, part], diag.at[c], in_sem.at[c, 1]),
            pltpu.make_async_copy(load_hbm.at[:, :, part], f.at[c], in_sem.at[c, 2]),
        )

    for at in (0, 1, 2):
        for c in range(chunks):
            loads(c)[at].start()

    barrier = pltpu.get_barrier_semaphore()
    count = 0
    for there, device in near:
        count = count + there.astype(jnp.int32)

    zero_col = jnp.zeros((PAD, LANES), jnp.float32)
    for slot in range(2):
        for c in range(chunks):
            for y in (0, ny + 1):
                u[slot, c, y] = jnp.zeros(u.shape[3:], jnp.float32)

    @pl.loop(1, ny + 1)
    def _(y):
        for slot in range(2):
            for c in range(chunks):
                u[slot, c, y, 0:PAD, :] = zero_col
                u[slot, c, y, PAD + nx : 2 * PAD + nx, :] = zero_col

    @pl.loop(0, my + 2 * DEPTH)
    def _(y):
        zero_row = jnp.zeros(cu.shape[3:], jnp.float32)
        for c in range(chunks):
            cu[0, c, y] = zero_row
            cu[1, c, y] = zero_row
            cl[c, y] = zero_row
            cw[c, y] = zero_row

    for there, device in near:

        @pl.when(there)
        def _():
            pl.semaphore_signal(barrier, inc=1, device_id=device, device_id_type=MESH)

    pl.semaphore_wait(barrier, count)

    def fine_copy(k, c, side, device):
        p, o = k % 2, side ^ 1
        if side < 2:
            src = u.at[p, c, 1 if side == 0 else ny, fine_x]
            dst = u.at[p, c, ny + 1 if side == 0 else 0, fine_x]
        else:
            src = col_out.at[p, c, side - 2]
            dst = col_in.at[p, c, o - 2]
        return pltpu.make_async_remote_copy(
            src_ref=src, dst_ref=dst, send_sem=send_sem.at[p, c, side], recv_sem=recv_sem.at[p, c, o],
            device_id=device, device_id_type=MESH,
        )

    def send_fine(k, c):
        p = k % 2

        @pl.loop(0, ny, unroll=8)
        def _(y):
            col_out[p, c, 0, pl.ds(y, 1), :] = u[p, c, 1 + y, PAD : PAD + 1, :]
            col_out[p, c, 1, pl.ds(y, 1), :] = u[p, c, 1 + y, PAD + nx - 1 : PAD + nx, :]

        for side in (2, 3, 0, 1):
            there, device = near[side]

            @pl.when(there)
            def _():
                fine_copy(k, c, side, device).start()

    def wait_fine(k, c):
        p = k % 2
        for side in (0, 1, 2, 3):
            there, device = near[side]

            @pl.when(there)
            def _():
                fine_copy(k, c, side, device).wait_send()
                fine_copy(k, c, side ^ 1, device).wait_recv()
                if side >= 2:
                    at = PAD - 1 if side == 2 else PAD + nx

                    @pl.loop(0, ny, unroll=8)
                    def _(y):
                        u[p, c, 1 + y, at : at + 1, :] = col_in[p, c, side - 2, pl.ds(y, 1), :]

    def cross(ref, y, x, rows):
        middle = [ref[y + i - 1, pl.ds(x, 8), :] for i in range(rows + 2)]
        return [
            (
                middle[i + 1],
                (middle[i] + middle[i + 2])
                + (ref[y + i, pl.ds(x - 1, 8), :] + ref[y + i, pl.ds(x + 1, 8), :]),
            )
            for i in range(rows)
        ]

    def sweep_fine(k, c):
        src, dst, ff, ww = u.at[k % 2, c], u.at[(k + 1) % 2, c], f.at[c], w.at[c]
        rows = 4

        @pl.loop(0, ny // rows)
        def _(g):
            y = g * rows
            for x in range(0, nx, 8):
                for i, (here, total) in enumerate(cross(src, y + 1, PAD + x, rows)):
                    new = (1.0 - OMEGA) * here + ww[y + i, pl.ds(x, 8), :] * (ff[y + i, pl.ds(x, 8), :] + total)
                    dst[y + 1 + i, pl.ds(PAD + x, 8), :] = new

    def halve(slot):
        return pair[slot, pl.ds(0, mx, stride=2), :] + pair[slot, pl.ds(1, mx, stride=2), :]

    def prepare(c):
        @pl.loop(0, my)
        def _(j):
            y = 2 * j
            for x in range(0, nx, 8):
                part = pl.ds(x, 8)
                m0, m1 = diag[c, y, part, :], diag[c, y + 1, part, :]
                pair[c, part, :] = m0 + m1
                d0, d1 = 4.0 + m0, 4.0 + m1
                diag[c, y, part, :] = d0
                diag[c, y + 1, part, :] = d1
                w[c, y, part, :] = OMEGA / d0
                w[c, y + 1, part, :] = OMEGA / d1
            cw[c, DEPTH + j, CX : CX + mx, :] = OMEGA / (4.0 + 0.5 * halve(c))

    def restrict(k, c):
        src = u.at[k % 2, c]

        @pl.loop(0, my)
        def _(j):
            y = 2 * j
            for x in range(0, nx, 8):
                part = pl.ds(x, 8)
                both = [
                    f[c, y + i, part, :] + total - diag[c, y + i, part, :] * here
                    for i, (here, total) in enumerate(cross(src, y + 1, PAD + x, 2))
                ]
                pair[c, part, :] = both[0] + both[1]
            cl[c, DEPTH + j, CX : CX + mx, :] = 0.5 * halve(c)

    def coarse_ref(slot, c):
        return (cw.at[c], cl.at[c])[slot] if slot < 2 else cu.at[0, c]

    def coarse_copy(slot, c, side, device):
        o = side ^ 1
        if side < 2:
            src = coarse_ref(slot, c).at[pl.ds(DEPTH if side == 0 else my, DEPTH), pl.ds(CX - PAD, wide)]
            dst = crow_in.at[slot, c, o]
        else:
            src = ccol_out.at[slot, c, side - 2]
            dst = ccol_in.at[slot, c, o - 2]
        return pltpu.make_async_remote_copy(
            src_ref=src, dst_ref=dst, send_sem=csend_sem.at[slot, c, side], recv_sem=crecv_sem.at[slot, c, o],
            device_id=device, device_id_type=MESH,
        )

    def send_columns(slot, c):
        ref = coarse_ref(slot, c)

        @pl.loop(0, my, unroll=8)
        def _(y):
            ccol_out[slot, c, 0, pl.ds(y * DEPTH, DEPTH), :] = ref[DEPTH + y, CX : CX + DEPTH, :]
            ccol_out[slot, c, 1, pl.ds(y * DEPTH, DEPTH), :] = ref[DEPTH + y, CX + mx - DEPTH : CX + mx, :]

        for side in (2, 3):
            there, device = near[side]

            @pl.when(there)
            def _():
                coarse_copy(slot, c, side, device).start()

    def columns_then_rows(slot, c):
        ref = coarse_ref(slot, c)
        for side in (2, 3):
            there, device = near[side]

            @pl.when(there)
            def _():
                coarse_copy(slot, c, side, device).wait_send()
                coarse_copy(slot, c, side ^ 1, device).wait_recv()
                at = CX - DEPTH if side == 2 else CX + mx

                @pl.loop(0, my, unroll=8)
                def _(y):
                    ref[DEPTH + y, at : at + DEPTH, :] = ccol_in[slot, c, side - 2, pl.ds(y * DEPTH, DEPTH), :]

        for side in (0, 1):
            there, device = near[side]

            @pl.when(there)
            def _():
                coarse_copy(slot, c, side, device).start()

    def wait_rows(slot, c):
        ref = coarse_ref(slot, c)
        for side in (0, 1):
            there, device = near[side]
            at = 0 if side == 0 else DEPTH + my

            @pl.when(there)
            def _():
                coarse_copy(slot, c, side, device).wait_send()
                coarse_copy(slot, c, side ^ 1, device).wait_recv()
                for i in range(DEPTH):
                    ref[at + i, pl.ds(CX - PAD, wide), :] = crow_in[slot, c, side, i]

    def sweep_coarse(s, c):
        src, dst, ff, ww = cu.at[s % 2, c], cu.at[(s + 1) % 2, c], cl.at[c], cw.at[c]
        rows = 2
        first, number = s + 1, my + 2 * DEPTH - 2 * (s + 1)

        @pl.loop(0, number // rows)
        def _(g):
            y = first + g * rows
            for x in range(CX - PAD, CX - PAD + wide, 8):
                for i, (here, total) in enumerate(cross(src, y, x, rows)):
                    part = pl.ds(x, 8)
                    dst[y + i, part, :] = (1.0 - OMEGA) * here + ww[y + i, part, :] * (ff[y + i, part, :] + total)

    def first_coarse(c):
        @pl.loop(0, my + 2 * DEPTH)
        def _(y):
            part = pl.ds(CX - PAD, wide)
            cu[0, c, y, part, :] = cw[c, y, part, :] * cl[c, y, part, :]

    def correct(k, c):
        @pl.loop(0, my)
        def _(j):
            add = cu[0, c, DEPTH + j, CX : CX + mx, :]
            for i in range(2):
                for odd in range(2):
                    part = pl.ds(PAD + odd, mx, stride=2)
                    u[(k + 1) % 2, c, 1 + 2 * j + i, part, :] = u[k % 2, c, 1 + 2 * j + i, part, :] + add

    def leave(k, c):
        src = u.at[k % 2, c]
        rows = 4

        @pl.loop(0, ny // rows)
        def _(g):
            y = g * rows
            for x in range(0, nx, 8):
                part = pl.ds(x, 8)
                for i, (here, total) in enumerate(cross(src, y + 1, PAD + x, rows)):
                    w[c, y + i, part, :] = f[c, y + i, part, :] + total - diag[c, y + i, part, :] * here

    both = range(chunks)
    for c in both:
        loads(c)[0].wait()
        send_fine(0, c)
    for c in both:
        loads(c)[1].wait()
        prepare(c)
        send_columns(0, c)
    for c in both:
        loads(c)[2].wait()
    k = 0
    for sweep in range(BEFORE):
        for c in both:
            wait_fine(k, c)
            sweep_fine(k, c)
            send_fine(k + 1, c)
            if sweep == 0:
                columns_then_rows(0, c)
            if sweep == 1:
                wait_rows(0, c)
        k += 1
    for c in both:
        wait_fine(k, c)
        restrict(k, c)
        send_columns(1, c)
    for c in both:
        columns_then_rows(1, c)
    rounds = (INNER - 1) // DEPTH
    for turn in range(rounds):
        for c in both:
            wait_rows(1 + turn, c)
            if turn == 0:
                first_coarse(c)
            for s in range(DEPTH):
                sweep_coarse(s, c)
            if turn < rounds - 1:
                send_columns(2 + turn, c)
            else:
                correct(k, c)
                send_fine(k + 1, c)
        if turn < rounds - 1:
            for c in both:
                columns_then_rows(2 + turn, c)
    k += 1
    for sweep in range(AFTER):
        for c in both:
            wait_fine(k, c)
            sweep_fine(k, c)
            send_fine(k + 1, c)
        k += 1
    for c in both:
        wait_fine(k, c)
        leave(k, c)


def store_kernel(u, w, sol_hbm, rem_hbm, out_sem):
    chunks, ny, nx = w.shape[:3]
    final = (BEFORE + 1 + AFTER) % 2
    copies = []
    for c in range(chunks):
        part = pl.ds(c * LANES, LANES)
        copies.append(pltpu.make_async_copy(u.at[final, c, pl.ds(1, ny), pl.ds(PAD, nx)], sol_hbm.at[:, :, part], out_sem.at[c, 0]))
        copies.append(pltpu.make_async_copy(w.at[c], rem_hbm.at[:, :, part], out_sem.at[c, 1]))
    for copy in copies:
        copy.start()
    for copy in copies:
        copy.wait()


def solution(mesh):
    bands, lanes = mesh.shape["band"], mesh.shape["lane"]

    def on_device(load_terms, start_values, reaction_rate):
        ny, nx, layers = load_terms.shape
        chunks = layers // LANES
        my, mx = ny // 2, nx // 2
        slots = 1 + (INNER - 1) // DEPTH
        f32 = jnp.float32
        vmem = lambda *shape: pltpu.VMEM(shape + (LANES,), f32)
        dma = lambda *shape: pltpu.SemaphoreType.DMA(shape)
        u, w = pl.pallas_call(
            functools.partial(kernel, bands, lanes),
            out_shape=[vmem(2, chunks, ny + 2, nx + 2 * PAD), vmem(chunks, ny, nx)],
            in_specs=[pl.BlockSpec(memory_space=pl.ANY)] * 3,
            out_specs=[pl.BlockSpec(memory_space=pltpu.VMEM)] * 2,
            scratch_shapes=[
                vmem(chunks, ny, nx),
                vmem(chunks, ny, nx),
                vmem(chunks, nx),
                vmem(2, chunks, my + 2 * DEPTH, mx + 2 * CX),
                vmem(chunks, my + 2 * DEPTH, mx + 2 * CX),
                vmem(chunks, my + 2 * DEPTH, mx + 2 * CX),
                vmem(2, chunks, 2, ny),
                vmem(2, chunks, 2, ny),
                vmem(slots, chunks, 2, my * DEPTH),
                vmem(slots, chunks, 2, my * DEPTH),
                vmem(slots, chunks, 2, DEPTH, mx + 2 * PAD),
                dma(chunks, 3),
                dma(2, chunks, 4),
                dma(2, chunks, 4),
                dma(slots, chunks, 4),
                dma(slots, chunks, 4),
            ],
            compiler_params=pltpu.CompilerParams(
                collective_id=0, has_side_effects=True, vmem_limit_bytes=46 * 1024 * 1024
            ),
        )(load_terms, start_values, reaction_rate)
        return pl.pallas_call(
            store_kernel,
            out_shape=[jax.ShapeDtypeStruct(load_terms.shape, f32)] * 2,
            in_specs=[pl.BlockSpec(memory_space=pltpu.VMEM)] * 2,
            out_specs=[pl.BlockSpec(memory_space=pl.ANY)] * 2,
            scratch_shapes=[dma(chunks, 2)],
            compiler_params=pltpu.CompilerParams(vmem_limit_bytes=1024 * 1024),
        )(pltpu.with_memory_space_constraint(u, pltpu.VMEM), pltpu.with_memory_space_constraint(w, pltpu.VMEM))

    placed = P("band", "lane", None)
    return jax.shard_map(
        on_device, mesh=mesh, in_specs=(placed,) * 3, out_specs=(placed, placed), check_vma=False
    )
```

```python
import functools

import jax
import jax.numpy as jnp
from jax import lax
from jax.experimental import pallas as pl
from jax.experimental.pallas import tpu as pltpu
from jax.sharding import PartitionSpec as P

BEFORE = 3
AFTER = 2
INNER = 13
OMEGA = 0.8
LANES = 128
DEPTH = 4
ROUNDS = (INNER - 1) // DEPTH
DEPTHS = (DEPTH,) * ROUNDS + (DEPTH + 1,)
PAD = 8
CX = 16
RY = DEPTH + 1
FINAL = (BEFORE + AFTER) % 2
MESH = pl.DeviceIdType.MESH


def corner_rows(depth):
    return -(-depth * (depth - 1) // 8) * 8


def opposite(side):
    return side ^ 1 if side < 4 else 11 - side


def kernel(
    bands, lanes, load_hbm, start_hbm, rate_hbm, u, w,
    f, diag, pair, cu, cl, cw, col_out, col_in, ccol_out, ccol_in, crow_in, corner_in,
    in_sem, send_sem, recv_sem, csend_sem, crecv_sem,
):
    ny, nx = f.shape[1], f.shape[2]
    my, mx = ny // 2, nx // 2
    chunks = f.shape[0]
    both = range(chunks)
    band, lane = lax.axis_index("band"), lax.axis_index("lane")
    near = [
        (band > 0, {"band": band - 1}),
        (band < bands - 1, {"band": band + 1}),
        (lane > 0, {"lane": lane - 1}),
        (lane < lanes - 1, {"lane": lane + 1}),
    ]
    for side in range(2):
        for across in range(2, 4):
            near.append((near[side][0] & near[across][0], near[side][1] | near[across][1]))
    fine_x = pl.ds(PAD, nx)

    def loads(c):
        part = pl.ds(c * LANES, LANES)
        return (
            pltpu.make_async_copy(start_hbm.at[:, :, part], u.at[0, c, pl.ds(1, ny), fine_x], in_sem.at[c, 0]),
            pltpu.make_async_copy(rate_hbm.at[:, :, part], diag.at[c], in_sem.at[c, 1]),
            pltpu.make_async_copy(load_hbm.at[:, :, part], f.at[c], in_sem.at[c, 2]),
        )

    barrier = pltpu.get_barrier_semaphore()
    count = 0
    for there, device in near:
        count = count + there.astype(jnp.int32)

    for at in (0, 1, 2):
        for c in both:
            loads(c)[at].start()

    zero = jnp.zeros((8, LANES), jnp.float32)
    for slot in range(2):
        for c in both:
            for y in (0, ny + 1):
                u[slot, c, y] = jnp.zeros(u.shape[3:], jnp.float32)

    for there, device in near:

        @pl.when(there)
        def _():
            pl.semaphore_signal(barrier, inc=1, device_id=device, device_id_type=MESH)

    @pl.loop(1, ny + 1)
    def _(y):
        for slot in range(2):
            for c in both:
                u[slot, c, y, 0:PAD, :] = zero
                u[slot, c, y, PAD + nx : 2 * PAD + nx, :] = zero

    @pl.loop(0, my + 2 * RY)
    def _(y):
        zero_row = jnp.zeros(cu.shape[3:], jnp.float32)
        for c in both:
            cu[0, c, y] = zero_row
            cu[1, c, y] = zero_row
            cl[c, y] = zero_row
            cw[c, y] = zero_row

    pl.semaphore_wait(barrier, count)

    def fine_copy(k, c, side, device):
        p, o = k % 2, opposite(side)
        if side < 2:
            src = u.at[p, c, 1 if side == 0 else ny, fine_x]
            dst = u.at[p, c, ny + 1 if side == 0 else 0, fine_x]
        else:
            src = col_out.at[p, c, side - 2]
            dst = col_in.at[p, c, o - 2]
        return pltpu.make_async_remote_copy(
            src_ref=src, dst_ref=dst, send_sem=send_sem.at[p, c, side], recv_sem=recv_sem.at[p, c, o],
            device_id=device, device_id_type=MESH,
        )

    def start_fine(k, c, sides):
        for side in sides:
            there, device = near[side]

            @pl.when(there)
            def _():
                fine_copy(k, c, side, device).start()

    def send_fine(k, c):
        p = k % 2
        start_fine(k, c, (0, 1))

        @pl.loop(0, ny, unroll=8)
        def _(y):
            col_out[p, c, 0, pl.ds(y, 1), :] = u[p, c, 1 + y, PAD : PAD + 1, :]
            col_out[p, c, 1, pl.ds(y, 1), :] = u[p, c, 1 + y, PAD + nx - 1 : PAD + nx, :]

        start_fine(k, c, (2, 3))

    def wait_fine(k, c):
        p = k % 2
        for side in (2, 3, 0, 1):
            there, device = near[side]

            @pl.when(there)
            def _():
                fine_copy(k, c, side, device).wait_send()
                fine_copy(k, c, opposite(side), device).wait_recv()
                if side >= 2:
                    at = PAD - 1 if side == 2 else PAD + nx

                    @pl.loop(0, ny, unroll=8)
                    def _(y):
                        u[p, c, 1 + y, at : at + 1, :] = col_in[p, c, side - 2, pl.ds(y, 1), :]

    def cross(ref, y, x, rows):
        middle = [ref[y + i - 1, pl.ds(x, 8), :] for i in range(rows + 2)]
        return [
            (
                middle[i + 1],
                (middle[i] + middle[i + 2])
                + (ref[y + i, pl.ds(x - 1, 8), :] + ref[y + i, pl.ds(x + 1, 8), :]),
            )
            for i in range(rows)
        ]

    def over(first, last, rows, body):
        groups = (last - first) // rows

        @pl.loop(0, groups)
        def _(g):
            body(first + g * rows, rows)

        if (last - first) % rows:
            body(first + groups * rows, (last - first) % rows)

    def outer(step, c):
        edges = (0, nx - 8)
        over(0, ny, 4, lambda y, rows: step(c, y, edges, rows))
        for y in (0, ny - 1):
            step(c, y, range(8, nx - 8, 8), 1)

    def inner(step, c):
        over(1, ny - 1, 4, lambda y, rows: step(c, y, range(8, nx - 8, 8), rows))

    def smooth(k):
        def step(c, y, xs, rows):
            src, dst, ff, ww = u.at[k % 2, c], u.at[(k + 1) % 2, c], f.at[c], w.at[c]
            for x in xs:
                for i, (here, total) in enumerate(cross(src, y + 1, PAD + x, rows)):
                    new = (1.0 - OMEGA) * here + ww[y + i, pl.ds(x, 8), :] * (ff[y + i, pl.ds(x, 8), :] + total)
                    dst[y + 1 + i, pl.ds(PAD + x, 8), :] = new

        return step

    def leave(k):
        def step(c, y, xs, rows):
            src = u.at[k % 2, c]
            for x in xs:
                part = pl.ds(x, 8)
                for i, (here, total) in enumerate(cross(src, y + 1, PAD + x, rows)):
                    w[c, y + i, part, :] = f[c, y + i, part, :] + total - diag[c, y + i, part, :] * here

        return step

    def halve(slot):
        return pair[slot, pl.ds(0, mx, stride=2), :] + pair[slot, pl.ds(1, mx, stride=2), :]

    def prepare(c):
        @pl.loop(0, my)
        def _(j):
            y = 2 * j
            for x in range(0, nx, 8):
                part = pl.ds(x, 8)
                m0, m1 = diag[c, y, part, :], diag[c, y + 1, part, :]
                pair[c, part, :] = m0 + m1
                d0, d1 = 4.0 + m0, 4.0 + m1
                diag[c, y, part, :] = d0
                diag[c, y + 1, part, :] = d1
                w[c, y, part, :] = OMEGA / d0
                w[c, y + 1, part, :] = OMEGA / d1
            cw[c, RY + j, CX : CX + mx, :] = OMEGA / (4.0 + 0.5 * halve(c))

    def restrict(k, c, first, last):
        src = u.at[k % 2, c]

        @pl.loop(first, last)
        def _(j):
            y = 2 * j
            for x in range(0, nx, 8):
                part = pl.ds(x, 8)
                both = [
                    f[c, y + i, part, :] + total - diag[c, y + i, part, :] * here
                    for i, (here, total) in enumerate(cross(src, y + 1, PAD + x, 2))
                ]
                pair[c, part, :] = both[0] + both[1]
            cl[c, RY + j, CX : CX + mx, :] = 0.5 * halve(c)

    def coarse_ref(slot, c):
        return (cw.at[c], cl.at[c])[slot] if slot < 2 else cu.at[0, c]

    def coarse_copy(slot, c, side, device):
        d, o = DEPTHS[slot], opposite(side)
        if side < 2:
            src = coarse_ref(slot, c).at[pl.ds(RY if side == 0 else RY + my - d, d), pl.ds(CX, mx)]
            dst = crow_in.at[slot, c, o, pl.ds(0, d)]
        elif side < 4:
            src = ccol_out.at[slot, c, side - 2, pl.ds(0, my * d)]
            dst = ccol_in.at[slot, c, o - 2, pl.ds(0, my * d)]
        else:
            number = corner_rows(d)
            src = ccol_out.at[slot, c, side % 2, pl.ds(0 if side < 6 else my * d - number, number)]
            dst = corner_in.at[slot, c, o - 4, pl.ds(0, number)]
        return pltpu.make_async_remote_copy(
            src_ref=src, dst_ref=dst, send_sem=csend_sem.at[slot, c, side], recv_sem=crecv_sem.at[slot, c, o],
            device_id=device, device_id_type=MESH,
        )

    def start_coarse(slot, c, sides):
        for side in sides:
            there, device = near[side]

            @pl.when(there)
            def _():
                coarse_copy(slot, c, side, device).start()

    def send_rows(slot, c):
        start_coarse(slot, c, (0, 1))

    def send_columns(slot, c):
        ref, d = coarse_ref(slot, c), DEPTHS[slot]

        @pl.loop(0, my, unroll=8)
        def _(y):
            ccol_out[slot, c, 0, pl.ds(y * d, d), :] = ref[RY + y, CX : CX + d, :]
            ccol_out[slot, c, 1, pl.ds(y * d, d), :] = ref[RY + y, CX + mx - d : CX + mx, :]

        start_coarse(slot, c, (4, 5, 6, 7, 2, 3))

    def wait_coarse(slot, c):
        ref, d = coarse_ref(slot, c), DEPTHS[slot]
        number = corner_rows(d)
        for side in range(8):
            there, device = near[side]

            @pl.when(there)
            def _():
                coarse_copy(slot, c, side, device).wait_send()
                coarse_copy(slot, c, opposite(side), device).wait_recv()
                if side < 2:
                    for i in range(d):
                        ref[(RY - d if side == 0 else RY + my) + i, pl.ds(CX, mx), :] = crow_in[slot, c, side, i]
                elif side < 4:
                    at = CX - d if side == 2 else CX + mx

                    @pl.loop(0, my, unroll=8)
                    def _(y):
                        ref[RY + y, at : at + d, :] = ccol_in[slot, c, side - 2, pl.ds(y * d, d), :]
                else:
                    at = CX - d if side % 2 == 0 else CX + mx
                    for i in range(1, d):
                        row, start = (RY - i, number - i * d) if side < 6 else (RY + my + i - 1, (i - 1) * d)
                        ref[row, at : at + d, :] = corner_in[slot, c, side - 4, start : start + d, :]

    coarse_x = range(CX - DEPTH, CX + mx + DEPTH, 8)

    def sweep_coarse(s, c, first, last):
        src, dst, ff, ww = cu.at[s % 2, c], cu.at[(s + 1) % 2, c], cl.at[c], cw.at[c]

        def step(y, rows):
            for x in coarse_x:
                for i, (here, total) in enumerate(cross(src, y, x, rows)):
                    part = pl.ds(x, 8)
                    dst[y + i, part, :] = (1.0 - OMEGA) * here + ww[y + i, part, :] * (ff[y + i, part, :] + total)

        over(RY + first, RY + last, 2, step)

    def first_coarse(c):
        @pl.loop(RY - DEPTH, RY + my + DEPTH)
        def _(y):
            for x in coarse_x:
                part = pl.ds(x, 8)
                cu[0, c, y, part, :] = cw[c, y, part, :] * cl[c, y, part, :]

    def correct(k, c):
        p = k % 2

        def rows(add, ys):
            for y in ys:
                for odd in range(2):
                    part = pl.ds(PAD + odd, mx, stride=2)
                    u[p, c, y, part, :] = u[p, c, y, part, :] + add

        @pl.loop(0, my)
        def _(j):
            y = 1 + 2 * j
            rows(cu[0, c, RY + j, CX : CX + mx, :], (y, y + 1))
            for at, beside in ((PAD - 1, CX - 1), (PAD + nx, CX + mx)):
                add = cu[0, c, RY + j, beside : beside + 1, :]
                for i in range(2):
                    u[p, c, y + i, at : at + 1, :] = u[p, c, y + i, at : at + 1, :] + add

        rows(cu[0, c, RY - 1, CX : CX + mx, :], (0,))
        rows(cu[0, c, RY + my, CX : CX + mx, :], (ny + 1,))

    for c in both:
        loads(c)[0].wait()
        send_fine(0, c)
    for c in both:
        loads(c)[1].wait()
        prepare(c)
        send_rows(0, c)
        send_columns(0, c)
    for c in both:
        loads(c)[2].wait()
    for k in range(BEFORE):
        for c in both:
            wait_fine(k, c)
            outer(smooth(k), c)
            send_fine(k + 1, c)
            inner(smooth(k), c)
    k = BEFORE
    for c in both:
        wait_fine(k, c)
        restrict(k, c, 0, DEPTH)
        restrict(k, c, my - DEPTH, my)
        send_rows(1, c)
        restrict(k, c, DEPTH, my - DEPTH)
        send_columns(1, c)
    for turn in range(ROUNDS):
        slot = 1 + turn
        for c in both:
            if turn == 0:
                wait_coarse(0, c)
            wait_coarse(slot, c)
            if turn == 0:
                first_coarse(c)
            reach = DEPTHS[slot] - 1
            for s in range(DEPTH - 1):
                sweep_coarse(s, c, s - reach, my + reach - s)
            if turn < ROUNDS - 1:
                d = DEPTHS[slot + 1]
                sweep_coarse(DEPTH - 1, c, 0, d)
                sweep_coarse(DEPTH - 1, c, my - d, my)
                send_rows(slot + 1, c)
                sweep_coarse(DEPTH - 1, c, d, my - d)
                send_columns(slot + 1, c)
            else:
                sweep_coarse(DEPTH - 1, c, -1, my + 1)
                correct(k, c)
                outer(smooth(k), c)
                send_fine(k + 1, c)
                inner(smooth(k), c)
    for k in range(BEFORE + 1, BEFORE + AFTER):
        for c in both:
            wait_fine(k, c)
            outer(smooth(k), c)
            send_fine(k + 1, c)
            inner(smooth(k), c)
            if k == BEFORE + AFTER - 1:
                inner(leave(k + 1), c)
    for c in both:
        wait_fine(BEFORE + AFTER, c)
        outer(leave(BEFORE + AFTER), c)


def store_kernel(u, w, sol_hbm, rem_hbm, out_sem):
    chunks, ny, nx = w.shape[:3]
    copies = []
    for c in range(chunks):
        part = pl.ds(c * LANES, LANES)
        values = u.at[FINAL, c, pl.ds(1, ny), pl.ds(PAD, nx)]
        copies.append(pltpu.make_async_copy(values, sol_hbm.at[:, :, part], out_sem.at[c, 0]))
        copies.append(pltpu.make_async_copy(w.at[c], rem_hbm.at[:, :, part], out_sem.at[c, 1]))
    for copy in copies:
        copy.start()
    for copy in copies:
        copy.wait()


def solution(mesh):
    bands, lanes = mesh.shape["band"], mesh.shape["lane"]

    def on_device(load_terms, start_values, reaction_rate):
        ny, nx, layers = load_terms.shape
        chunks = layers // LANES
        my, mx = ny // 2, nx // 2
        slots = ROUNDS + 1
        f32 = jnp.float32
        vmem = lambda *shape: pltpu.VMEM(shape + (LANES,), f32)
        dma = lambda *shape: pltpu.SemaphoreType.DMA(shape)
        u, w = pl.pallas_call(
            functools.partial(kernel, bands, lanes),
            out_shape=[vmem(2, chunks, ny + 2, nx + 2 * PAD), vmem(chunks, ny, nx)],
            in_specs=[pl.BlockSpec(memory_space=pl.ANY)] * 3,
            out_specs=[pl.BlockSpec(memory_space=pltpu.VMEM)] * 2,
            scratch_shapes=[
                vmem(chunks, ny, nx),
                vmem(chunks, ny, nx),
                vmem(chunks, nx),
                vmem(2, chunks, my + 2 * RY, mx + 2 * CX),
                vmem(chunks, my + 2 * RY, mx + 2 * CX),
                vmem(chunks, my + 2 * RY, mx + 2 * CX),
                vmem(2, chunks, 2, ny),
                vmem(2, chunks, 2, ny),
                vmem(slots, chunks, 2, my * RY),
                vmem(slots, chunks, 2, my * RY),
                vmem(slots, chunks, 2, RY, mx),
                vmem(slots, chunks, 4, corner_rows(RY)),
                dma(chunks, 3),
                dma(2, chunks, 4),
                dma(2, chunks, 4),
                dma(slots, chunks, 8),
                dma(slots, chunks, 8),
            ],
            compiler_params=pltpu.CompilerParams(
                collective_id=0, has_side_effects=True, vmem_limit_bytes=46 * 1024 * 1024
            ),
        )(load_terms, start_values, reaction_rate)
        in_vmem = lambda x: pltpu.with_memory_space_constraint(x, pltpu.VMEM)
        return pl.pallas_call(
            store_kernel,
            out_shape=[jax.ShapeDtypeStruct(load_terms.shape, f32)] * 2,
            in_specs=[pl.BlockSpec(memory_space=pltpu.VMEM)] * 2,
            out_specs=[pl.BlockSpec(memory_space=pl.ANY)] * 2,
            scratch_shapes=[dma(chunks, 2)],
            compiler_params=pltpu.CompilerParams(vmem_limit_bytes=1024 * 1024),
        )(in_vmem(u), in_vmem(w))

    placed = P("band", "lane", None)
    return jax.shard_map(
        on_device, mesh=mesh, in_specs=(placed,) * 3, out_specs=(placed, placed), check_vma=False
    )
```

```python
import functools

import jax
import jax.numpy as jnp
from jax import lax
from jax.experimental import pallas as pl
from jax.experimental.pallas import tpu as pltpu
from jax.sharding import PartitionSpec as P

BEFORE = 3
AFTER = 2
INNER = 13
OMEGA = 0.8
LANES = 128
DEPTH = 4
ROUNDS = (INNER - 1) // DEPTH
DEPTHS = (DEPTH,) * ROUNDS + (DEPTH + 1,)
PAD = 8
CX = 16
RY = DEPTH + 1
FINAL = (BEFORE + AFTER) % 2
MESH = pl.DeviceIdType.MESH


def corner_rows(depth):
    return -(-depth * (depth - 1) // 8) * 8


def opposite(side):
    return side ^ 1 if side < 4 else 11 - side


def kernel(
    bands, lanes, load_hbm, start_hbm, rate_hbm, u, w,
    f, diag, pair, cu, cl, cw, col_out, col_in, ccol_out, ccol_in, crow_in, corner_in,
    in_sem, send_sem, recv_sem, csend_sem, crecv_sem,
):
    ny, nx = f.shape[1], f.shape[2]
    my, mx = ny // 2, nx // 2
    chunks = f.shape[0]
    both = range(chunks)
    band, lane = lax.axis_index("band"), lax.axis_index("lane")
    near = [
        (band > 0, {"band": band - 1}),
        (band < bands - 1, {"band": band + 1}),
        (lane > 0, {"lane": lane - 1}),
        (lane < lanes - 1, {"lane": lane + 1}),
    ]
    for side in range(2):
        for across in range(2, 4):
            near.append((near[side][0] & near[across][0], near[side][1] | near[across][1]))
    fine_x = pl.ds(PAD, nx)

    def loads(c):
        part = pl.ds(c * LANES, LANES)
        return (
            pltpu.make_async_copy(start_hbm.at[:, :, part], u.at[0, c, pl.ds(1, ny), fine_x], in_sem.at[c, 0]),
            pltpu.make_async_copy(rate_hbm.at[:, :, part], diag.at[c], in_sem.at[c, 1]),
            pltpu.make_async_copy(load_hbm.at[:, :, part], f.at[c], in_sem.at[c, 2]),
        )

    barrier = pltpu.get_barrier_semaphore()
    count = 0
    for there, device in near:
        count = count + there.astype(jnp.int32)

    for at in (0, 1, 2):
        for c in both:
            loads(c)[at].start()

    zero = jnp.zeros((8, LANES), jnp.float32)
    for slot in range(2):
        for c in both:
            for y in (0, ny + 1):
                u[slot, c, y] = jnp.zeros(u.shape[3:], jnp.float32)

    for there, device in near:

        @pl.when(there)
        def _():
            pl.semaphore_signal(barrier, inc=1, device_id=device, device_id_type=MESH)

    pl.semaphore_wait(barrier, count)

    def fine_copy(k, c, side, device):
        p, o = k % 2, opposite(side)
        if side < 2:
            src = u.at[p, c, 1 if side == 0 else ny, fine_x]
            dst = u.at[p, c, ny + 1 if side == 0 else 0, fine_x]
        else:
            src = col_out.at[p, c, side - 2]
            dst = col_in.at[p, c, o - 2]
        return pltpu.make_async_remote_copy(
            src_ref=src, dst_ref=dst, send_sem=send_sem.at[p, c, side], recv_sem=recv_sem.at[p, c, o],
            device_id=device, device_id_type=MESH,
        )

    def start_fine(k, c, sides):
        for side in sides:
            there, device = near[side]

            @pl.when(there)
            def _():
                fine_copy(k, c, side, device).start()

    def send_fine(k, c):
        p = k % 2
        start_fine(k, c, (0, 1))

        @pl.loop(0, ny, unroll=8)
        def _(y):
            col_out[p, c, 0, pl.ds(y, 1), :] = u[p, c, 1 + y, PAD : PAD + 1, :]
            col_out[p, c, 1, pl.ds(y, 1), :] = u[p, c, 1 + y, PAD + nx - 1 : PAD + nx, :]

        start_fine(k, c, (2, 3))

    def wait_fine(k, c):
        p = k % 2
        for side in (2, 3, 0, 1):
            there, device = near[side]

            @pl.when(there)
            def _():
                fine_copy(k, c, side, device).wait_send()
                fine_copy(k, c, opposite(side), device).wait_recv()
                if side >= 2:
                    at = PAD - 1 if side == 2 else PAD + nx

                    @pl.loop(0, ny, unroll=8)
                    def _(y):
                        u[p, c, 1 + y, at : at + 1, :] = col_in[p, c, side - 2, pl.ds(y, 1), :]

    def cross(ref, y, x, rows):
        middle = [ref[y + i - 1, pl.ds(x, 8), :] for i in range(rows + 2)]
        return [
            (
                middle[i + 1],
                (middle[i] + middle[i + 2])
                + (ref[y + i, pl.ds(x - 1, 8), :] + ref[y + i, pl.ds(x + 1, 8), :]),
            )
            for i in range(rows)
        ]

    def over(first, last, rows, body):
        groups = (last - first) // rows

        @pl.loop(0, groups)
        def _(g):
            body(first + g * rows, rows)

        if (last - first) % rows:
            body(first + groups * rows, (last - first) % rows)

    def outer(step, c):
        edges = (0, nx - 8)
        over(0, ny, 8, lambda y, rows: step(c, y, edges, rows))
        for y in (0, ny - 1):
            step(c, y, range(8, nx - 8, 8), 1)

    def inner(step, c):
        over(1, ny - 1, 4, lambda y, rows: step(c, y, range(8, nx - 8, 8), rows))

    def smooth(k):
        def step(c, y, xs, rows):
            src, dst, ff, ww = u.at[k % 2, c], u.at[(k + 1) % 2, c], f.at[c], w.at[c]
            for x in xs:
                for i, (here, total) in enumerate(cross(src, y + 1, PAD + x, rows)):
                    new = (1.0 - OMEGA) * here + ww[y + i, pl.ds(x, 8), :] * (ff[y + i, pl.ds(x, 8), :] + total)
                    dst[y + 1 + i, pl.ds(PAD + x, 8), :] = new

        return step

    def leave(k):
        def step(c, y, xs, rows):
            src = u.at[k % 2, c]
            for x in xs:
                part = pl.ds(x, 8)
                for i, (here, total) in enumerate(cross(src, y + 1, PAD + x, rows)):
                    w[c, y + i, part, :] = f[c, y + i, part, :] + total - diag[c, y + i, part, :] * here

        return step

    def halve(slot):
        return pair[slot, pl.ds(0, mx, stride=2), :] + pair[slot, pl.ds(1, mx, stride=2), :]

    def prepare(c):
        @pl.loop(0, my)
        def _(j):
            y = 2 * j
            for x in range(0, nx, 8):
                part = pl.ds(x, 8)
                m0, m1 = diag[c, y, part, :], diag[c, y + 1, part, :]
                pair[2 * c, part, :] = m0 + m1
                d0, d1 = 4.0 + m0, 4.0 + m1
                diag[c, y, part, :] = d0
                diag[c, y + 1, part, :] = d1
                w[c, y, part, :] = OMEGA / d0
                w[c, y + 1, part, :] = OMEGA / d1
            cw[c, RY + j, CX : CX + mx, :] = OMEGA / (4.0 + 0.5 * halve(2 * c))

    def restrict(k, c, first, last):
        src = u.at[k % 2, c]

        def step(j, rows):
            y = 2 * j
            for x in range(0, nx, 8):
                part = pl.ds(x, 8)
                defect = [
                    f[c, y + i, part, :] + total - diag[c, y + i, part, :] * here
                    for i, (here, total) in enumerate(cross(src, y + 1, PAD + x, 2 * rows))
                ]
                for i in range(rows):
                    pair[2 * c + i, part, :] = defect[2 * i] + defect[2 * i + 1]
            for i in range(rows):
                cl[c, RY + j + i, CX : CX + mx, :] = 0.5 * halve(2 * c + i)

        over(first, last, 2, step)

    def coarse_ref(slot, c):
        return (cw.at[c], cl.at[c])[slot] if slot < 2 else cu.at[0, c]

    def coarse_copy(slot, c, side, device):
        d, o = DEPTHS[slot], opposite(side)
        if side < 2:
            src = coarse_ref(slot, c).at[pl.ds(RY if side == 0 else RY + my - d, d), pl.ds(CX, mx)]
            dst = crow_in.at[slot, c, o, pl.ds(0, d)]
        elif side < 4:
            src = ccol_out.at[slot, c, side - 2, pl.ds(0, my * d)]
            dst = ccol_in.at[slot, c, o - 2, pl.ds(0, my * d)]
        else:
            number = corner_rows(d)
            src = ccol_out.at[slot, c, side % 2, pl.ds(0 if side < 6 else my * d - number, number)]
            dst = corner_in.at[slot, c, o - 4, pl.ds(0, number)]
        return pltpu.make_async_remote_copy(
            src_ref=src, dst_ref=dst, send_sem=csend_sem.at[slot, c, side], recv_sem=crecv_sem.at[slot, c, o],
            device_id=device, device_id_type=MESH,
        )

    def start_coarse(slot, c, sides):
        for side in sides:
            there, device = near[side]

            @pl.when(there)
            def _():
                coarse_copy(slot, c, side, device).start()

    def send_rows(slot, c):
        start_coarse(slot, c, (0, 1))

    def send_columns(slot, c):
        ref, d = coarse_ref(slot, c), DEPTHS[slot]

        @pl.loop(0, my, unroll=8)
        def _(y):
            ccol_out[slot, c, 0, pl.ds(y * d, d), :] = ref[RY + y, CX : CX + d, :]
            ccol_out[slot, c, 1, pl.ds(y * d, d), :] = ref[RY + y, CX + mx - d : CX + mx, :]

        start_coarse(slot, c, (4, 5, 6, 7, 2, 3))

    def wait_coarse(slot, c):
        ref, d = coarse_ref(slot, c), DEPTHS[slot]
        number = corner_rows(d)
        for side in range(8):
            there, device = near[side]

            @pl.when(there)
            def _():
                coarse_copy(slot, c, side, device).wait_send()
                coarse_copy(slot, c, opposite(side), device).wait_recv()
                if side < 2:
                    for i in range(d):
                        ref[(RY - d if side == 0 else RY + my) + i, pl.ds(CX, mx), :] = crow_in[slot, c, side, i]
                elif side < 4:
                    at = CX - d if side == 2 else CX + mx

                    @pl.loop(0, my, unroll=8)
                    def _(y):
                        ref[RY + y, at : at + d, :] = ccol_in[slot, c, side - 2, pl.ds(y * d, d), :]
                else:
                    at = CX - d if side % 2 == 0 else CX + mx
                    for i in range(1, d):
                        row, start = (RY - i, number - i * d) if side < 6 else (RY + my + i - 1, (i - 1) * d)
                        ref[row, at : at + d, :] = corner_in[slot, c, side - 4, start : start + d, :]

    coarse_x = range(CX - DEPTH, CX + mx + DEPTH, 8)

    def sweep_coarse(s, c, first, last):
        src, dst, ff, ww = cu.at[s % 2, c], cu.at[(s + 1) % 2, c], cl.at[c], cw.at[c]

        def step(y, rows):
            for x in coarse_x:
                for i, (here, total) in enumerate(cross(src, y, x, rows)):
                    part = pl.ds(x, 8)
                    dst[y + i, part, :] = (1.0 - OMEGA) * here + ww[y + i, part, :] * (ff[y + i, part, :] + total)

        over(RY + first, RY + last, 4, step)

    def first_coarse(c):
        @pl.loop(RY - DEPTH, RY + my + DEPTH, unroll=4)
        def _(y):
            for x in coarse_x:
                part = pl.ds(x, 8)
                cu[0, c, y, part, :] = cw[c, y, part, :] * cl[c, y, part, :]

    def correct(k, c, outside):
        p = k % 2
        near_x, far_x = (0, mx - 8), range(8, mx - 8, 8)

        def block(j, ys, xs):
            for x in xs:
                add = cu[0, c, RY + j, pl.ds(CX + x, 8), :]
                for y in ys:
                    for odd in range(2):
                        part = pl.ds(PAD + 2 * x + odd, 8, stride=2)
                        u[p, c, y, part, :] = u[p, c, y, part, :] + add

        if not outside:

            @pl.loop(1, my - 1, unroll=2)
            def _(j):
                block(j, (1 + 2 * j, 2 + 2 * j), far_x)

            return

        @pl.loop(0, my, unroll=2)
        def _(j):
            y = 1 + 2 * j
            block(j, (y, y + 1), near_x)
            for at, beside in ((PAD - 1, CX - 1), (PAD + nx, CX + mx)):
                add = cu[0, c, RY + j, beside : beside + 1, :]
                for i in range(2):
                    u[p, c, y + i, at : at + 1, :] = u[p, c, y + i, at : at + 1, :] + add

        block(-1, (0,), range(0, mx, 8))
        block(0, (1, 2), far_x)
        block(my - 1, (ny - 1, ny), far_x)
        block(my, (ny + 1,), range(0, mx, 8))

    def clear():
        @pl.loop(1, ny + 1)
        def _(y):
            for slot in range(2):
                for c in both:
                    u[slot, c, y, 0:PAD, :] = zero
                    u[slot, c, y, PAD + nx : 2 * PAD + nx, :] = zero

        @pl.loop(0, my + 2 * RY)
        def _(y):
            zero_row = jnp.zeros(cu.shape[3:], jnp.float32)
            for c in both:
                cu[0, c, y] = zero_row
                cu[1, c, y] = zero_row
                cl[c, y] = zero_row
                cw[c, y] = zero_row

    for c in both:
        loads(c)[0].wait()
        send_fine(0, c)
    clear()
    for c in both:
        loads(c)[1].wait()
        prepare(c)
        send_rows(0, c)
    for c in both:
        loads(c)[2].wait()
    for k in range(BEFORE):
        for c in both:
            wait_fine(k, c)
            outer(smooth(k), c)
            send_fine(k + 1, c)
            if c == chunks - 1 and k < chunks:
                send_columns(0, k)
            inner(smooth(k), c)
    k = BEFORE
    for c in both:
        wait_fine(k, c)
        restrict(k, c, 0, DEPTH)
        restrict(k, c, my - DEPTH, my)
        send_rows(1, c)
        restrict(k, c, DEPTH, my - DEPTH)
        send_columns(1, c)
    for turn in range(ROUNDS):
        slot = 1 + turn
        for c in both:
            if turn == 0:
                wait_coarse(0, c)
            wait_coarse(slot, c)
            if turn == 0:
                first_coarse(c)
            reach = DEPTHS[slot] - 1
            for s in range(DEPTH - 1):
                sweep_coarse(s, c, s - reach, my + reach - s)
            if turn < ROUNDS - 1:
                d = DEPTHS[slot + 1]
                sweep_coarse(DEPTH - 1, c, 0, d)
                sweep_coarse(DEPTH - 1, c, my - d, my)
                send_rows(slot + 1, c)
                sweep_coarse(DEPTH - 1, c, d, my - d)
                send_columns(slot + 1, c)
            else:
                sweep_coarse(DEPTH - 1, c, -1, my + 1)
                correct(k, c, True)
                outer(smooth(k), c)
                send_fine(k + 1, c)
                correct(k, c, False)
                inner(smooth(k), c)
    for k in range(BEFORE + 1, BEFORE + AFTER):
        for c in both:
            wait_fine(k, c)
            outer(smooth(k), c)
            send_fine(k + 1, c)
            inner(smooth(k), c)
            if k == BEFORE + AFTER - 1:
                inner(leave(k + 1), c)
    for c in both:
        wait_fine(BEFORE + AFTER, c)
        outer(leave(BEFORE + AFTER), c)


def store_kernel(u, w, sol_hbm, rem_hbm, out_sem):
    chunks, ny, nx = w.shape[:3]
    copies = []
    for c in range(chunks):
        part = pl.ds(c * LANES, LANES)
        values = u.at[FINAL, c, pl.ds(1, ny), pl.ds(PAD, nx)]
        copies.append(pltpu.make_async_copy(values, sol_hbm.at[:, :, part], out_sem.at[c, 0]))
        copies.append(pltpu.make_async_copy(w.at[c], rem_hbm.at[:, :, part], out_sem.at[c, 1]))
    for copy in copies:
        copy.start()
    for copy in copies:
        copy.wait()


def solution(mesh):
    bands, lanes = mesh.shape["band"], mesh.shape["lane"]

    def on_device(load_terms, start_values, reaction_rate):
        ny, nx, layers = load_terms.shape
        chunks = layers // LANES
        my, mx = ny // 2, nx // 2
        slots = ROUNDS + 1
        f32 = jnp.float32
        vmem = lambda *shape: pltpu.VMEM(shape + (LANES,), f32)
        dma = lambda *shape: pltpu.SemaphoreType.DMA(shape)
        u, w = pl.pallas_call(
            functools.partial(kernel, bands, lanes),
            out_shape=[vmem(2, chunks, ny + 2, nx + 2 * PAD), vmem(chunks, ny, nx)],
            in_specs=[pl.BlockSpec(memory_space=pl.ANY)] * 3,
            out_specs=[pl.BlockSpec(memory_space=pltpu.VMEM)] * 2,
            scratch_shapes=[
                vmem(chunks, ny, nx),
                vmem(chunks, ny, nx),
                vmem(2 * chunks, nx),
                vmem(2, chunks, my + 2 * RY, mx + 2 * CX),
                vmem(chunks, my + 2 * RY, mx + 2 * CX),
                vmem(chunks, my + 2 * RY, mx + 2 * CX),
                vmem(2, chunks, 2, ny),
                vmem(2, chunks, 2, ny),
                vmem(slots, chunks, 2, my * RY),
                vmem(slots, chunks, 2, my * RY),
                vmem(slots, chunks, 2, RY, mx),
                vmem(slots, chunks, 4, corner_rows(RY)),
                dma(chunks, 3),
                dma(2, chunks, 4),
                dma(2, chunks, 4),
                dma(slots, chunks, 8),
                dma(slots, chunks, 8),
            ],
            compiler_params=pltpu.CompilerParams(
                collective_id=0, has_side_effects=True, vmem_limit_bytes=46 * 1024 * 1024
            ),
        )(load_terms, start_values, reaction_rate)
        in_vmem = lambda x: pltpu.with_memory_space_constraint(x, pltpu.VMEM)
        return pl.pallas_call(
            store_kernel,
            out_shape=[jax.ShapeDtypeStruct(load_terms.shape, f32)] * 2,
            in_specs=[pl.BlockSpec(memory_space=pltpu.VMEM)] * 2,
            out_specs=[pl.BlockSpec(memory_space=pl.ANY)] * 2,
            scratch_shapes=[dma(chunks, 2)],
            compiler_params=pltpu.CompilerParams(vmem_limit_bytes=1024 * 1024),
        )(in_vmem(u), in_vmem(w))

    placed = P("band", "lane", None)
    return jax.shard_map(
        on_device, mesh=mesh, in_specs=(placed,) * 3, out_specs=(placed, placed), check_vma=False
    )
```

```python
import functools

import jax
import jax.numpy as jnp
from jax import lax
from jax.experimental import pallas as pl
from jax.experimental.pallas import tpu as pltpu
from jax.sharding import PartitionSpec as P

BEFORE = 3
AFTER = 2
INNER = 13
OMEGA = 0.8
LANES = 128
DEPTH = 3
ROUNDS = (INNER - 1) // DEPTH
DEPTHS = (DEPTH,) * ROUNDS + (DEPTH + 1,)
PAD = 8
CX = 16
RY = DEPTH + 1
FINAL = (BEFORE + AFTER) % 2
MESH = pl.DeviceIdType.MESH


def corner_rows(depth):
    return -(-depth * (depth - 1) // 8) * 8


def opposite(side):
    return side ^ 1 if side < 4 else 11 - side


def kernel(
    bands, lanes, load_hbm, start_hbm, rate_hbm, u, w,
    f, diag, pair, cu, cl, cw, col_out, col_in, ccol_out, ccol_in, crow_in, corner_in,
    in_sem, send_sem, recv_sem, csend_sem, crecv_sem,
):
    ny, nx = f.shape[1], f.shape[2]
    my, mx = ny // 2, nx // 2
    chunks = f.shape[0]
    both = range(chunks)
    band, lane = lax.axis_index("band"), lax.axis_index("lane")
    near = [
        (band > 0, {"band": band - 1}),
        (band < bands - 1, {"band": band + 1}),
        (lane > 0, {"lane": lane - 1}),
        (lane < lanes - 1, {"lane": lane + 1}),
    ]
    for side in range(2):
        for across in range(2, 4):
            near.append((near[side][0] & near[across][0], near[side][1] | near[across][1]))
    fine_x = pl.ds(PAD, nx)

    def loads(c):
        part = pl.ds(c * LANES, LANES)
        return (
            pltpu.make_async_copy(start_hbm.at[:, :, part], u.at[0, c, pl.ds(1, ny), fine_x], in_sem.at[c, 0]),
            pltpu.make_async_copy(rate_hbm.at[:, :, part], diag.at[c], in_sem.at[c, 1]),
            pltpu.make_async_copy(load_hbm.at[:, :, part], f.at[c], in_sem.at[c, 2]),
        )

    barrier = pltpu.get_barrier_semaphore()
    count = 0
    for there, device in near:
        count = count + there.astype(jnp.int32)

    for at in (0, 1, 2):
        for c in both:
            loads(c)[at].start()

    zero = jnp.zeros((8, LANES), jnp.float32)
    for slot in range(2):
        for c in both:
            for y in (0, ny + 1):
                u[slot, c, y] = jnp.zeros(u.shape[3:], jnp.float32)

    for there, device in near:

        @pl.when(there)
        def _():
            pl.semaphore_signal(barrier, inc=1, device_id=device, device_id_type=MESH)

    pl.semaphore_wait(barrier, count)

    def fine_copy(k, c, side, device):
        p, o = k % 2, opposite(side)
        if side < 2:
            src = u.at[p, c, 1 if side == 0 else ny, fine_x]
            dst = u.at[p, c, ny + 1 if side == 0 else 0, fine_x]
        else:
            src = col_out.at[p, c, side - 2]
            dst = col_in.at[p, c, o - 2]
        return pltpu.make_async_remote_copy(
            src_ref=src, dst_ref=dst, send_sem=send_sem.at[p, c, side], recv_sem=recv_sem.at[p, c, o],
            device_id=device, device_id_type=MESH,
        )

    def start_fine(k, c, sides):
        for side in sides:
            there, device = near[side]

            @pl.when(there)
            def _():
                fine_copy(k, c, side, device).start()

    def send_columns_fine(k, c):
        p = k % 2

        @pl.loop(0, ny, unroll=8)
        def _(y):
            col_out[p, c, 0, pl.ds(y, 1), :] = u[p, c, 1 + y, PAD : PAD + 1, :]
            col_out[p, c, 1, pl.ds(y, 1), :] = u[p, c, 1 + y, PAD + nx - 1 : PAD + nx, :]

        start_fine(k, c, (2, 3))

    def finish_fine(k, c):
        for side in range(4):
            there, device = near[side]

            @pl.when(there)
            def _():
                fine_copy(k, c, side, device).wait_send()

    def wait_fine(k, c):
        p = k % 2
        if k not in (0, BEFORE + 1):
            finish_fine(k - 1, c)
        for side in (2, 3, 0, 1):
            there, device = near[side]

            @pl.when(there)
            def _():
                fine_copy(k, c, opposite(side), device).wait_recv()
                if side >= 2:
                    at = PAD - 1 if side == 2 else PAD + nx

                    @pl.loop(0, ny, unroll=8)
                    def _(y):
                        u[p, c, 1 + y, at : at + 1, :] = col_in[p, c, side - 2, pl.ds(y, 1), :]

    def cross(ref, y, x, rows):
        middle = [ref[y + i - 1, pl.ds(x, 8), :] for i in range(rows + 2)]
        return [
            (
                middle[i + 1],
                (middle[i] + middle[i + 2])
                + (ref[y + i, pl.ds(x - 1, 8), :] + ref[y + i, pl.ds(x + 1, 8), :]),
            )
            for i in range(rows)
        ]

    def over(first, last, rows, body):
        groups = (last - first) // rows

        @pl.loop(0, groups)
        def _(g):
            body(first + g * rows, rows)

        if (last - first) % rows:
            body(first + groups * rows, (last - first) % rows)

    def outer_rows(step, c):
        for y in (0, ny - 1):
            step(c, y, range(0, nx, 8), 1)

    def outer_columns(step, c):
        over(1, ny - 1, 8, lambda y, rows: step(c, y, (0, nx - 8), rows))

    def inner(step, c):
        over(1, ny - 1, 4, lambda y, rows: step(c, y, range(8, nx - 8, 8), rows))

    def smooth(k):
        def step(c, y, xs, rows):
            src, dst, ff, ww = u.at[k % 2, c], u.at[(k + 1) % 2, c], f.at[c], w.at[c]
            for x in xs:
                for i, (here, total) in enumerate(cross(src, y + 1, PAD + x, rows)):
                    new = (1.0 - OMEGA) * here + ww[y + i, pl.ds(x, 8), :] * (ff[y + i, pl.ds(x, 8), :] + total)
                    dst[y + 1 + i, pl.ds(PAD + x, 8), :] = new

        return step

    def leave(k):
        def step(c, y, xs, rows):
            src = u.at[k % 2, c]
            for x in xs:
                part = pl.ds(x, 8)
                for i, (here, total) in enumerate(cross(src, y + 1, PAD + x, rows)):
                    w[c, y + i, part, :] = f[c, y + i, part, :] + total - diag[c, y + i, part, :] * here

        return step

    def sweep(k, c, between=None):
        step = smooth(k)
        outer_rows(step, c)
        start_fine(k + 1, c, (0, 1))
        outer_columns(step, c)
        send_columns_fine(k + 1, c)
        if between is not None:
            between()
        inner(step, c)

    def halve(slot):
        return pair[slot, pl.ds(0, mx, stride=2), :] + pair[slot, pl.ds(1, mx, stride=2), :]

    def prepare(c):
        @pl.loop(0, my)
        def _(j):
            y = 2 * j
            for x in range(0, nx, 8):
                part = pl.ds(x, 8)
                m0, m1 = diag[c, y, part, :], diag[c, y + 1, part, :]
                pair[2 * c, part, :] = m0 + m1
                d0, d1 = 4.0 + m0, 4.0 + m1
                diag[c, y, part, :] = d0
                diag[c, y + 1, part, :] = d1
                w[c, y, part, :] = OMEGA / d0
                w[c, y + 1, part, :] = OMEGA / d1
            cw[c, RY + j, CX : CX + mx, :] = OMEGA / (4.0 + 0.5 * halve(2 * c))

    def restrict(k, c, first, last):
        src = u.at[k % 2, c]

        def step(j, rows):
            y = 2 * j
            for x in range(0, nx, 8):
                part = pl.ds(x, 8)
                defect = [
                    f[c, y + i, part, :] + total - diag[c, y + i, part, :] * here
                    for i, (here, total) in enumerate(cross(src, y + 1, PAD + x, 2 * rows))
                ]
                for i in range(rows):
                    pair[2 * c + i, part, :] = defect[2 * i] + defect[2 * i + 1]
            for i in range(rows):
                cl[c, RY + j + i, CX : CX + mx, :] = 0.5 * halve(2 * c + i)

        over(first, last, 2, step)

    def coarse_ref(slot, c):
        return (cw.at[c], cl.at[c])[slot] if slot < 2 else cu.at[DEPTH * (slot - 1) % 2, c]

    def coarse_copy(slot, c, side, device):
        d, o = DEPTHS[slot], opposite(side)
        if side < 2:
            src = coarse_ref(slot, c).at[pl.ds(RY if side == 0 else RY + my - d, d), pl.ds(CX, mx)]
            dst = crow_in.at[slot, c, o, pl.ds(0, d)]
        elif side < 4:
            src = ccol_out.at[slot, c, side - 2, pl.ds(0, my * d)]
            dst = ccol_in.at[slot, c, o - 2, pl.ds(0, my * d)]
        else:
            number = corner_rows(d)
            src = ccol_out.at[slot, c, side % 2, pl.ds(0 if side < 6 else my * d - number, number)]
            dst = corner_in.at[slot, c, o - 4, pl.ds(0, number)]
        return pltpu.make_async_remote_copy(
            src_ref=src, dst_ref=dst, send_sem=csend_sem.at[slot, c, side], recv_sem=crecv_sem.at[slot, c, o],
            device_id=device, device_id_type=MESH,
        )

    def start_coarse(slot, c, sides):
        for side in sides:
            there, device = near[side]

            @pl.when(there)
            def _():
                coarse_copy(slot, c, side, device).start()

    def send_rows(slot, c):
        start_coarse(slot, c, (0, 1))

    def send_columns(slot, c):
        ref, d = coarse_ref(slot, c), DEPTHS[slot]

        @pl.loop(0, my, unroll=8)
        def _(y):
            ccol_out[slot, c, 0, pl.ds(y * d, d), :] = ref[RY + y, CX : CX + d, :]
            ccol_out[slot, c, 1, pl.ds(y * d, d), :] = ref[RY + y, CX + mx - d : CX + mx, :]

        start_coarse(slot, c, (4, 5, 6, 7, 2, 3))

    def wait_coarse(slot, c):
        ref, d = coarse_ref(slot, c), DEPTHS[slot]
        number = corner_rows(d)
        for side in range(8):
            there, device = near[side]

            @pl.when(there)
            def _():
                coarse_copy(slot, c, opposite(side), device).wait_recv()
                if side < 2:
                    for i in range(d):
                        ref[(RY - d if side == 0 else RY + my) + i, pl.ds(CX, mx), :] = crow_in[slot, c, side, i]
                elif side < 4:
                    at = CX - d if side == 2 else CX + mx

                    @pl.loop(0, my, unroll=8)
                    def _(y):
                        ref[RY + y, at : at + d, :] = ccol_in[slot, c, side - 2, pl.ds(y * d, d), :]
                else:
                    at = CX - d if side % 2 == 0 else CX + mx
                    for i in range(1, d):
                        row, start = (RY - i, number - i * d) if side < 6 else (RY + my + i - 1, (i - 1) * d)
                        ref[row, at : at + d, :] = corner_in[slot, c, side - 4, start : start + d, :]

    def finish_coarse(slot, c, sides):
        for side in sides:
            there, device = near[side]

            @pl.when(there)
            def _():
                coarse_copy(slot, c, side, device).wait_send()

    coarse_x = range(CX - DEPTH, CX + mx + DEPTH, 8)

    def sweep_coarse(s, c, first, last):
        src, dst, ff, ww = cu.at[s % 2, c], cu.at[(s + 1) % 2, c], cl.at[c], cw.at[c]

        def step(y, rows):
            for x in coarse_x:
                for i, (here, total) in enumerate(cross(src, y, x, rows)):
                    part = pl.ds(x, 8)
                    dst[y + i, part, :] = (1.0 - OMEGA) * here + ww[y + i, part, :] * (ff[y + i, part, :] + total)

        over(RY + first, RY + last, 4, step)

    def first_coarse(c):
        @pl.loop(RY - DEPTH, RY + my + DEPTH, unroll=4)
        def _(y):
            for x in coarse_x:
                part = pl.ds(x, 8)
                cu[0, c, y, part, :] = cw[c, y, part, :] * cl[c, y, part, :]

    def correct(k, c, outside):
        p = k % 2
        near_x, far_x = (0, mx - 8), range(8, mx - 8, 8)

        def block(j, ys, xs):
            for x in xs:
                add = cu[0, c, RY + j, pl.ds(CX + x, 8), :]
                for y in ys:
                    for odd in range(2):
                        part = pl.ds(PAD + 2 * x + odd, 8, stride=2)
                        u[p, c, y, part, :] = u[p, c, y, part, :] + add

        if not outside:

            @pl.loop(1, my - 1, unroll=2)
            def _(j):
                block(j, (1 + 2 * j, 2 + 2 * j), far_x)

            return

        @pl.loop(0, my, unroll=2)
        def _(j):
            y = 1 + 2 * j
            block(j, (y, y + 1), near_x)
            for at, beside in ((PAD - 1, CX - 1), (PAD + nx, CX + mx)):
                add = cu[0, c, RY + j, beside : beside + 1, :]
                for i in range(2):
                    u[p, c, y + i, at : at + 1, :] = u[p, c, y + i, at : at + 1, :] + add

        block(-1, (0,), range(0, mx, 8))
        block(0, (1, 2), far_x)
        block(my - 1, (ny - 1, ny), far_x)
        block(my, (ny + 1,), range(0, mx, 8))

    def clear():
        @pl.loop(1, ny + 1)
        def _(y):
            for slot in range(2):
                for c in both:
                    u[slot, c, y, 0:PAD, :] = zero
                    u[slot, c, y, PAD + nx : 2 * PAD + nx, :] = zero

        @pl.loop(0, my + 2 * RY)
        def _(y):
            zero_row = jnp.zeros(cu.shape[3:], jnp.float32)
            for c in both:
                cu[0, c, y] = zero_row
                cu[1, c, y] = zero_row
                cl[c, y] = zero_row
                cw[c, y] = zero_row

    for c in both:
        loads(c)[0].wait()
        start_fine(0, c, (0, 1))
        send_columns_fine(0, c)
    clear()
    for c in both:
        loads(c)[1].wait()
        prepare(c)
        send_rows(0, c)
    for c in both:
        loads(c)[2].wait()
    for k in range(BEFORE):
        for c in both:
            wait_fine(k, c)
            sweep(k, c, functools.partial(send_columns, 0, k) if c == chunks - 1 and k < chunks else None)
    k = BEFORE
    for c in both:
        wait_fine(k, c)
        restrict(k, c, 0, DEPTH)
        restrict(k, c, my - DEPTH, my)
        send_rows(1, c)
        restrict(k, c, DEPTH, my - DEPTH)
        send_columns(1, c)
    for turn in range(ROUNDS):
        slot = 1 + turn
        for c in both:
            if turn == 0:
                wait_coarse(0, c)
            wait_coarse(slot, c)
            if turn == 0:
                first_coarse(c)
            reach, base = DEPTHS[slot] - 1, DEPTH * turn
            for s in range(DEPTH - 1):
                sweep_coarse(base + s, c, s - reach, my + reach - s)
                if s == 0 and turn > 0:
                    finish_coarse(slot, c, (0, 1))
            if turn < ROUNDS - 1:
                d = DEPTHS[slot + 1]
                sweep_coarse(base + DEPTH - 1, c, 0, d)
                sweep_coarse(base + DEPTH - 1, c, my - d, my)
                send_rows(slot + 1, c)
                sweep_coarse(base + DEPTH - 1, c, d, my - d)
                send_columns(slot + 1, c)
            else:
                sweep_coarse(base + DEPTH - 1, c, -1, my + 1)
                finish_fine(k, c)
                correct(k, c, True)
                sweep(k, c, functools.partial(correct, k, c, False))
    for k in range(BEFORE + 1, BEFORE + AFTER):
        for c in both:
            wait_fine(k, c)
            sweep(k, c)
            if k == BEFORE + AFTER - 1:
                inner(leave(k + 1), c)
    for c in both:
        wait_fine(BEFORE + AFTER, c)
        outer_rows(leave(BEFORE + AFTER), c)
        outer_columns(leave(BEFORE + AFTER), c)
    for c in both:
        finish_fine(BEFORE + AFTER, c)
        for slot in range(ROUNDS + 1):
            finish_coarse(slot, c, range(8) if slot < 2 else range(2, 8))


def store_kernel(u, w, sol_hbm, rem_hbm, out_sem):
    chunks, ny, nx = w.shape[:3]
    copies = []
    for c in range(chunks):
        part = pl.ds(c * LANES, LANES)
        values = u.at[FINAL, c, pl.ds(1, ny), pl.ds(PAD, nx)]
        copies.append(pltpu.make_async_copy(values, sol_hbm.at[:, :, part], out_sem.at[c, 0]))
        copies.append(pltpu.make_async_copy(w.at[c], rem_hbm.at[:, :, part], out_sem.at[c, 1]))
    for copy in copies:
        copy.start()
    for copy in copies:
        copy.wait()


def solution(mesh):
    bands, lanes = mesh.shape["band"], mesh.shape["lane"]

    def on_device(load_terms, start_values, reaction_rate):
        ny, nx, layers = load_terms.shape
        chunks = layers // LANES
        my, mx = ny // 2, nx // 2
        slots = ROUNDS + 1
        f32 = jnp.float32
        vmem = lambda *shape: pltpu.VMEM(shape + (LANES,), f32)
        dma = lambda *shape: pltpu.SemaphoreType.DMA(shape)
        u, w = pl.pallas_call(
            functools.partial(kernel, bands, lanes),
            out_shape=[vmem(2, chunks, ny + 2, nx + 2 * PAD), vmem(chunks, ny, nx)],
            in_specs=[pl.BlockSpec(memory_space=pl.ANY)] * 3,
            out_specs=[pl.BlockSpec(memory_space=pltpu.VMEM)] * 2,
            scratch_shapes=[
                vmem(chunks, ny, nx),
                vmem(chunks, ny, nx),
                vmem(2 * chunks, nx),
                vmem(2, chunks, my + 2 * RY, mx + 2 * CX),
                vmem(chunks, my + 2 * RY, mx + 2 * CX),
                vmem(chunks, my + 2 * RY, mx + 2 * CX),
                vmem(2, chunks, 2, ny),
                vmem(2, chunks, 2, ny),
                vmem(slots, chunks, 2, my * RY),
                vmem(slots, chunks, 2, my * RY),
                vmem(slots, chunks, 2, RY, mx),
                vmem(slots, chunks, 4, corner_rows(RY)),
                dma(chunks, 3),
                dma(2, chunks, 4),
                dma(2, chunks, 4),
                dma(slots, chunks, 8),
                dma(slots, chunks, 8),
            ],
            compiler_params=pltpu.CompilerParams(
                collective_id=0, has_side_effects=True, vmem_limit_bytes=46 * 1024 * 1024
            ),
        )(load_terms, start_values, reaction_rate)
        in_vmem = lambda x: pltpu.with_memory_space_constraint(x, pltpu.VMEM)
        return pl.pallas_call(
            store_kernel,
            out_shape=[jax.ShapeDtypeStruct(load_terms.shape, f32)] * 2,
            in_specs=[pl.BlockSpec(memory_space=pltpu.VMEM)] * 2,
            out_specs=[pl.BlockSpec(memory_space=pl.ANY)] * 2,
            scratch_shapes=[dma(chunks, 2)],
            compiler_params=pltpu.CompilerParams(vmem_limit_bytes=1024 * 1024),
        )(in_vmem(u), in_vmem(w))

    placed = P("band", "lane", None)
    return jax.shard_map(
        on_device, mesh=mesh, in_specs=(placed,) * 3, out_specs=(placed, placed), check_vma=False
    )
```

```python
import functools

import jax
import jax.numpy as jnp
from jax import lax
from jax.experimental import pallas as pl
from jax.experimental.pallas import tpu as pltpu
from jax.sharding import PartitionSpec as P

BEFORE = 3
AFTER = 2
INNER = 13
OMEGA = 0.8
LANES = 128
DEPTH = 3
ROUNDS = (INNER - 1) // DEPTH
DEPTHS = (DEPTH,) * ROUNDS + (DEPTH + 1,)
PAD = 8
CX = 16
RY = DEPTH + 1
FINAL = (BEFORE + AFTER) % 2
MESH = pl.DeviceIdType.MESH


def corner_rows(depth):
    return -(-depth * (depth - 1) // 8) * 8


def opposite(side):
    return side ^ 1 if side < 4 else 11 - side


def kernel(
    bands, lanes, load_hbm, start_hbm, rate_hbm, u, w,
    f, diag, pair, cu, cl, cw, col_out, col_in, ccol_out, ccol_in, crow_in, corner_in,
    in_sem, send_sem, recv_sem, csend_sem, crecv_sem,
):
    ny, nx = f.shape[1], f.shape[2]
    my, mx = ny // 2, nx // 2
    chunks = f.shape[0]
    both = range(chunks)
    band, lane = lax.axis_index("band"), lax.axis_index("lane")
    near = [
        (band > 0, {"band": band - 1}),
        (band < bands - 1, {"band": band + 1}),
        (lane > 0, {"lane": lane - 1}),
        (lane < lanes - 1, {"lane": lane + 1}),
    ]
    for side in range(2):
        for across in range(2, 4):
            near.append((near[side][0] & near[across][0], near[side][1] | near[across][1]))
    fine_x = pl.ds(PAD, nx)

    def loads(c):
        part = pl.ds(c * LANES, LANES)
        return (
            pltpu.make_async_copy(start_hbm.at[:, :, part], u.at[0, c, pl.ds(1, ny), fine_x], in_sem.at[c, 0]),
            pltpu.make_async_copy(rate_hbm.at[:, :, part], diag.at[c], in_sem.at[c, 1]),
            pltpu.make_async_copy(load_hbm.at[:, :, part], f.at[c], in_sem.at[c, 2]),
        )

    barrier = pltpu.get_barrier_semaphore()
    count = 0
    for there, device in near:
        count = count + there.astype(jnp.int32)

    for at in (0, 1, 2):
        for c in both:
            loads(c)[at].start()

    zero = jnp.zeros((8, LANES), jnp.float32)
    for slot in range(2):
        for c in both:
            for y in (0, ny + 1):
                u[slot, c, y] = jnp.zeros(u.shape[3:], jnp.float32)

    for there, device in near:

        @pl.when(there)
        def _():
            pl.semaphore_signal(barrier, inc=1, device_id=device, device_id_type=MESH)

    pl.semaphore_wait(barrier, count)

    def fine_copy(k, c, side, device):
        p, o = k % 2, opposite(side)
        if side < 2:
            src = u.at[p, c, 1 if side == 0 else ny, fine_x]
            dst = u.at[p, c, ny + 1 if side == 0 else 0, fine_x]
        else:
            src = col_out.at[p, c, side - 2]
            dst = col_in.at[p, c, o - 2]
        return pltpu.make_async_remote_copy(
            src_ref=src, dst_ref=dst, send_sem=send_sem.at[p, c, side], recv_sem=recv_sem.at[p, c, o],
            device_id=device, device_id_type=MESH,
        )

    def start_fine(k, c, sides):
        for side in sides:
            there, device = near[side]

            @pl.when(there)
            def _():
                fine_copy(k, c, side, device).start()

    def send_columns_fine(k, c):
        p = k % 2

        @pl.loop(0, ny, unroll=8)
        def _(y):
            col_out[p, c, 0, pl.ds(y, 1), :] = u[p, c, 1 + y, PAD : PAD + 1, :]
            col_out[p, c, 1, pl.ds(y, 1), :] = u[p, c, 1 + y, PAD + nx - 1 : PAD + nx, :]

        start_fine(k, c, (2, 3))

    def finish_fine(k, c):
        for side in range(4):
            there, device = near[side]

            @pl.when(there)
            def _():
                fine_copy(k, c, side, device).wait_send()

    def wait_fine(k, c):
        p = k % 2
        if k not in (0, BEFORE + 1):
            finish_fine(k - 1, c)
        for side in (2, 3, 0, 1):
            there, device = near[side]

            @pl.when(there)
            def _():
                fine_copy(k, c, opposite(side), device).wait_recv()
                if side >= 2:
                    at = PAD - 1 if side == 2 else PAD + nx

                    @pl.loop(0, ny, unroll=8)
                    def _(y):
                        u[p, c, 1 + y, at : at + 1, :] = col_in[p, c, side - 2, pl.ds(y, 1), :]

    def cross(ref, y, x, rows):
        middle = [ref[y + i - 1, pl.ds(x, 8), :] for i in range(rows + 2)]
        return [
            (
                middle[i + 1],
                (middle[i] + middle[i + 2])
                + (ref[y + i, pl.ds(x - 1, 8), :] + ref[y + i, pl.ds(x + 1, 8), :]),
            )
            for i in range(rows)
        ]

    def over(first, last, rows, body):
        groups = (last - first) // rows

        @pl.loop(0, groups)
        def _(g):
            body(first + g * rows, rows)

        if (last - first) % rows:
            body(first + groups * rows, (last - first) % rows)

    def outer_rows(step, c):
        for y in (0, ny - 1):
            step(c, y, range(0, nx, 8), 1)

    def outer_columns(step, c):
        over(1, ny - 1, 8, lambda y, rows: step(c, y, (0, nx - 8), rows))

    def inner(step, c):
        over(1, ny - 1, 4, lambda y, rows: step(c, y, range(8, nx - 8, 8), rows))

    def smooth(k):
        def step(c, y, xs, rows):
            src, dst, ff, ww = u.at[k % 2, c], u.at[(k + 1) % 2, c], f.at[c], w.at[c]
            for x in xs:
                for i, (here, total) in enumerate(cross(src, y + 1, PAD + x, rows)):
                    new = (1.0 - OMEGA) * here + ww[y + i, pl.ds(x, 8), :] * (ff[y + i, pl.ds(x, 8), :] + total)
                    dst[y + 1 + i, pl.ds(PAD + x, 8), :] = new

        return step

    def leave(k):
        def step(c, y, xs, rows):
            src = u.at[k % 2, c]
            for x in xs:
                part = pl.ds(x, 8)
                for i, (here, total) in enumerate(cross(src, y + 1, PAD + x, rows)):
                    w[c, y + i, part, :] = f[c, y + i, part, :] + total - diag[c, y + i, part, :] * here

        return step

    def sweep(k, c, between=None):
        step = smooth(k)
        outer_rows(step, c)
        start_fine(k + 1, c, (0, 1))
        outer_columns(step, c)
        send_columns_fine(k + 1, c)
        if between is not None:
            between()
        inner(step, c)

    def halve(slot):
        return pair[slot, pl.ds(0, mx, stride=2), :] + pair[slot, pl.ds(1, mx, stride=2), :]

    def prepare(c):
        @pl.loop(0, my)
        def _(j):
            y = 2 * j
            for x in range(0, nx, 8):
                part = pl.ds(x, 8)
                m0, m1 = diag[c, y, part, :], diag[c, y + 1, part, :]
                pair[2 * c, part, :] = m0 + m1
                d0, d1 = 4.0 + m0, 4.0 + m1
                diag[c, y, part, :] = d0
                diag[c, y + 1, part, :] = d1
                w[c, y, part, :] = OMEGA / d0
                w[c, y + 1, part, :] = OMEGA / d1
            cw[c, RY + j, CX : CX + mx, :] = OMEGA / (4.0 + 0.5 * halve(2 * c))

    def restrict(k, c, first, last):
        src = u.at[k % 2, c]

        def step(j, rows):
            y = 2 * j
            for x in range(0, nx, 8):
                part = pl.ds(x, 8)
                defect = [
                    f[c, y + i, part, :] + total - diag[c, y + i, part, :] * here
                    for i, (here, total) in enumerate(cross(src, y + 1, PAD + x, 2 * rows))
                ]
                for i in range(rows):
                    pair[2 * c + i, part, :] = defect[2 * i] + defect[2 * i + 1]
            for i in range(rows):
                cl[c, RY + j + i, CX : CX + mx, :] = 0.5 * halve(2 * c + i)

        over(first, last, 2, step)

    def coarse_ref(slot, c):
        return (cw.at[c], cl.at[c])[slot] if slot < 2 else cu.at[DEPTH * (slot - 1) % 2, c]

    def coarse_copy(slot, c, side, device):
        d, o = DEPTHS[slot], opposite(side)
        if side < 2:
            src = coarse_ref(slot, c).at[pl.ds(RY if side == 0 else RY + my - d, d), pl.ds(CX, mx)]
            dst = crow_in.at[slot, c, o, pl.ds(0, d)]
        elif side < 4:
            src = ccol_out.at[slot, c, side - 2, pl.ds(0, my * d)]
            dst = ccol_in.at[slot, c, o - 2, pl.ds(0, my * d)]
        else:
            number = corner_rows(d)
            src = ccol_out.at[slot, c, side % 2, pl.ds(0 if side < 6 else my * d - number, number)]
            dst = corner_in.at[slot, c, o - 4, pl.ds(0, number)]
        return pltpu.make_async_remote_copy(
            src_ref=src, dst_ref=dst, send_sem=csend_sem.at[slot, c, side], recv_sem=crecv_sem.at[slot, c, o],
            device_id=device, device_id_type=MESH,
        )

    def start_coarse(slot, c, sides):
        for side in sides:
            there, device = near[side]

            @pl.when(there)
            def _():
                coarse_copy(slot, c, side, device).start()

    def pack_columns(slot, c, y):
        ref, d = coarse_ref(slot, c), DEPTHS[slot]
        ccol_out[slot, c, 0, pl.ds(y * d, d), :] = ref[RY + y, CX : CX + d, :]
        ccol_out[slot, c, 1, pl.ds(y * d, d), :] = ref[RY + y, CX + mx - d : CX + mx, :]

    def send_rows(slot, c):
        d = DEPTHS[slot]
        for y in (*range(d), *range(my - d, my)):
            pack_columns(slot, c, y)
        start_coarse(slot, c, (4, 5, 6, 7, 0, 1))

    def send_columns(slot, c):
        d = DEPTHS[slot]

        @pl.loop(d, my - d, unroll=2)
        def _(y):
            pack_columns(slot, c, y)

        start_coarse(slot, c, (2, 3))

    def wait_coarse(slot, c):
        ref, d = coarse_ref(slot, c), DEPTHS[slot]
        number = corner_rows(d)
        for side in range(8):
            there, device = near[side]

            @pl.when(there)
            def _():
                coarse_copy(slot, c, opposite(side), device).wait_recv()
                if side < 2:
                    for i in range(d):
                        ref[(RY - d if side == 0 else RY + my) + i, pl.ds(CX, mx), :] = crow_in[slot, c, side, i]
                elif side < 4:
                    at = CX - d if side == 2 else CX + mx

                    @pl.loop(0, my, unroll=8)
                    def _(y):
                        ref[RY + y, at : at + d, :] = ccol_in[slot, c, side - 2, pl.ds(y * d, d), :]
                else:
                    at = CX - d if side % 2 == 0 else CX + mx
                    for i in range(1, d):
                        row, start = (RY - i, number - i * d) if side < 6 else (RY + my + i - 1, (i - 1) * d)
                        ref[row, at : at + d, :] = corner_in[slot, c, side - 4, start : start + d, :]

    def finish_coarse(slot, c, sides):
        for side in sides:
            there, device = near[side]

            @pl.when(there)
            def _():
                coarse_copy(slot, c, side, device).wait_send()

    coarse_x = range(CX - DEPTH, CX + mx + DEPTH, 8)

    def sweep_coarse(s, c, first, last):
        src, dst, ff, ww = cu.at[s % 2, c], cu.at[(s + 1) % 2, c], cl.at[c], cw.at[c]

        def step(y, rows):
            for x in coarse_x:
                for i, (here, total) in enumerate(cross(src, y, x, rows)):
                    part = pl.ds(x, 8)
                    dst[y + i, part, :] = (1.0 - OMEGA) * here + ww[y + i, part, :] * (ff[y + i, part, :] + total)

        over(RY + first, RY + last, 4, step)

    def first_coarse(c):
        @pl.loop(RY - DEPTH, RY + my + DEPTH, unroll=4)
        def _(y):
            for x in coarse_x:
                part = pl.ds(x, 8)
                cu[0, c, y, part, :] = cw[c, y, part, :] * cl[c, y, part, :]

    def correct(k, c, outside):
        p = k % 2
        near_x, far_x = (0, mx - 8), range(8, mx - 8, 8)

        def block(j, ys, xs):
            for x in xs:
                add = cu[0, c, RY + j, pl.ds(CX + x, 8), :]
                for y in ys:
                    for odd in range(2):
                        part = pl.ds(PAD + 2 * x + odd, 8, stride=2)
                        u[p, c, y, part, :] = u[p, c, y, part, :] + add

        if not outside:

            @pl.loop(1, my - 1, unroll=2)
            def _(j):
                block(j, (1 + 2 * j, 2 + 2 * j), far_x)

            return

        @pl.loop(0, my, unroll=2)
        def _(j):
            y = 1 + 2 * j
            block(j, (y, y + 1), near_x)
            for at, beside in ((PAD - 1, CX - 1), (PAD + nx, CX + mx)):
                add = cu[0, c, RY + j, beside : beside + 1, :]
                for i in range(2):
                    u[p, c, y + i, at : at + 1, :] = u[p, c, y + i, at : at + 1, :] + add

        block(-1, (0,), range(0, mx, 8))
        block(0, (1, 2), far_x)
        block(my - 1, (ny - 1, ny), far_x)
        block(my, (ny + 1,), range(0, mx, 8))

    def clear():
        @pl.loop(1, ny + 1)
        def _(y):
            for slot in range(2):
                for c in both:
                    u[slot, c, y, 0:PAD, :] = zero
                    u[slot, c, y, PAD + nx : 2 * PAD + nx, :] = zero

        @pl.loop(0, my + 2 * RY)
        def _(y):
            zero_row = jnp.zeros(cu.shape[3:], jnp.float32)
            for c in both:
                cu[0, c, y] = zero_row
                cu[1, c, y] = zero_row
                cl[c, y] = zero_row
                cw[c, y] = zero_row

    for c in both:
        loads(c)[0].wait()
        start_fine(0, c, (0, 1))
        send_columns_fine(0, c)
    clear()
    for c in both:
        loads(c)[1].wait()
        prepare(c)
        send_rows(0, c)
    for c in both:
        loads(c)[2].wait()
    for k in range(BEFORE):
        for c in both:
            wait_fine(k, c)
            sweep(k, c, functools.partial(send_columns, 0, k) if c == chunks - 1 and k < chunks else None)
    k = BEFORE
    for c in both:
        wait_fine(k, c)
        restrict(k, c, 0, DEPTH)
        restrict(k, c, my - DEPTH, my)
        send_rows(1, c)
        restrict(k, c, DEPTH, my - DEPTH)
        send_columns(1, c)
    for turn in range(ROUNDS):
        slot = 1 + turn
        for c in both:
            if turn == 0:
                wait_coarse(0, c)
            wait_coarse(slot, c)
            if turn == 0:
                first_coarse(c)
            reach, base = DEPTHS[slot] - 1, DEPTH * turn
            for s in range(DEPTH - 1):
                sweep_coarse(base + s, c, s - reach, my + reach - s)
                if s == 0 and turn > 0:
                    finish_coarse(slot, c, (0, 1))
            if turn < ROUNDS - 1:
                d = DEPTHS[slot + 1]
                sweep_coarse(base + DEPTH - 1, c, 0, d)
                sweep_coarse(base + DEPTH - 1, c, my - d, my)
                send_rows(slot + 1, c)
                sweep_coarse(base + DEPTH - 1, c, d, my - d)
                send_columns(slot + 1, c)
            else:
                sweep_coarse(base + DEPTH - 1, c, -1, my + 1)
                finish_fine(k, c)
                correct(k, c, True)
                sweep(k, c, functools.partial(correct, k, c, False))
    for k in range(BEFORE + 1, BEFORE + AFTER):
        for c in both:
            wait_fine(k, c)
            sweep(k, c)
            if k == BEFORE + AFTER - 1:
                inner(leave(k + 1), c)
    for c in both:
        wait_fine(BEFORE + AFTER, c)
        outer_rows(leave(BEFORE + AFTER), c)
        outer_columns(leave(BEFORE + AFTER), c)
    for c in both:
        finish_fine(BEFORE + AFTER, c)
        for slot in range(ROUNDS + 1):
            finish_coarse(slot, c, range(8) if slot < 2 else range(2, 8))


def store_kernel(u, w, sol_hbm, rem_hbm, out_sem):
    chunks, ny, nx = w.shape[:3]
    copies = []
    for c in range(chunks):
        part = pl.ds(c * LANES, LANES)
        values = u.at[FINAL, c, pl.ds(1, ny), pl.ds(PAD, nx)]
        copies.append(pltpu.make_async_copy(values, sol_hbm.at[:, :, part], out_sem.at[c, 0]))
        copies.append(pltpu.make_async_copy(w.at[c], rem_hbm.at[:, :, part], out_sem.at[c, 1]))
    for copy in copies:
        copy.start()
    for copy in copies:
        copy.wait()


def solution(mesh):
    bands, lanes = mesh.shape["band"], mesh.shape["lane"]

    def on_device(load_terms, start_values, reaction_rate):
        ny, nx, layers = load_terms.shape
        chunks = layers // LANES
        my, mx = ny // 2, nx // 2
        slots = ROUNDS + 1
        f32 = jnp.float32
        vmem = lambda *shape: pltpu.VMEM(shape + (LANES,), f32)
        dma = lambda *shape: pltpu.SemaphoreType.DMA(shape)
        u, w = pl.pallas_call(
            functools.partial(kernel, bands, lanes),
            out_shape=[vmem(2, chunks, ny + 2, nx + 2 * PAD), vmem(chunks, ny, nx)],
            in_specs=[pl.BlockSpec(memory_space=pl.ANY)] * 3,
            out_specs=[pl.BlockSpec(memory_space=pltpu.VMEM)] * 2,
            scratch_shapes=[
                vmem(chunks, ny, nx),
                vmem(chunks, ny, nx),
                vmem(2 * chunks, nx),
                vmem(2, chunks, my + 2 * RY, mx + 2 * CX),
                vmem(chunks, my + 2 * RY, mx + 2 * CX),
                vmem(chunks, my + 2 * RY, mx + 2 * CX),
                vmem(2, chunks, 2, ny),
                vmem(2, chunks, 2, ny),
                vmem(slots, chunks, 2, my * RY),
                vmem(slots, chunks, 2, my * RY),
                vmem(slots, chunks, 2, RY, mx),
                vmem(slots, chunks, 4, corner_rows(RY)),
                dma(chunks, 3),
                dma(2, chunks, 4),
                dma(2, chunks, 4),
                dma(slots, chunks, 8),
                dma(slots, chunks, 8),
            ],
            compiler_params=pltpu.CompilerParams(
                collective_id=0, has_side_effects=True, vmem_limit_bytes=46 * 1024 * 1024
            ),
        )(load_terms, start_values, reaction_rate)
        in_vmem = lambda x: pltpu.with_memory_space_constraint(x, pltpu.VMEM)
        return pl.pallas_call(
            store_kernel,
            out_shape=[jax.ShapeDtypeStruct(load_terms.shape, f32)] * 2,
            in_specs=[pl.BlockSpec(memory_space=pltpu.VMEM)] * 2,
            out_specs=[pl.BlockSpec(memory_space=pl.ANY)] * 2,
            scratch_shapes=[dma(chunks, 2)],
            compiler_params=pltpu.CompilerParams(vmem_limit_bytes=1024 * 1024),
        )(in_vmem(u), in_vmem(w))

    placed = P("band", "lane", None)
    return jax.shard_map(
        on_device, mesh=mesh, in_specs=(placed,) * 3, out_specs=(placed, placed), check_vma=False
    )
```
